32 devices in a mesh: parts: 2 (over x), blk: 16 (over z, y, core).
Axes of the slice: x: 2, y: 2, z: 4, core: 2. Of those that a mesh axis runs over, the one named last changes fastest.
Arguments:
- queries: bfloat16 [2048, 4096], P(('parts', 'blk')), parts along dimension 0, may hold values from -12 to 12
- keys: bfloat16 [2048, 512], P(('parts', 'blk')), parts along dimension 0, may hold values from -12 to 12
- values: bfloat16 [2048, 512], P(('parts', 'blk')), parts along dimension 0, may hold values from -6 to 6
- span_order: int32 [64], P('parts'), parts along dimension 0, may hold values from 0 to 31, as said below
Outputs:
- attended: bfloat16 [2048, 4096], P(('parts', 'blk')), parts along dimension 0
The draws below stay inside these ranges and needn't reach their ends.
There are 2 independent parts, one for each index of `parts`. The reference program is written for one: setup_inputs(seed, part) draws one part's arguments, and reference() takes and returns one part's arrays. A program takes and returns all parts, laid end to end along the dimension named above; each array names one. Nothing has to cross between parts.
Inputs may be any that keep to these rules, and one draw needn't show every extreme that they name: `span_order`: a permutation of the 32 blocks; slots 2i and 2i+1 hold blocks c and 31 - c for some c.
All inputs are finite; a program needn't handle non-finite values.
Results may differ from the reference program's by a relative error of at most 0.0065.
Values may be sent and summed in bfloat16 or wider, within the bound.
No kernel may reach another device: no remote copies, remote signals or barrier semaphores. Data moves between devices by JAX's collectives and lax.ppermute only.
A program may use at most 64 MiB of HBM per device.

```python
import jax
import jax.numpy as jnp
from jax import lax

HEADS = 32
KV_HEADS = 4
HEAD = 128
TOK_DEV = 64
SPANS = 32
TOKENS = 1024


def draw_queries(key, part):
    base = jax.random.normal(jax.random.fold_in(key, 13), (TOKENS, HEADS * HEAD), jnp.float32)
    return jnp.clip(base, -6.0, 6.0).astype(jnp.bfloat16)


def draw_keys(key, part):
    base = jax.random.normal(jax.random.fold_in(key, 23), (TOKENS, KV_HEADS * HEAD), jnp.float32)
    return jnp.clip(base, -6.0, 6.0).astype(jnp.bfloat16)


def draw_span_order(key, part):
    pairs = SPANS // 2
    owner = jax.random.permutation(jax.random.fold_in(key, 31), pairs)
    flips = jax.random.randint(jax.random.fold_in(key, 32), (pairs,), 0, 2)
    lower = owner
    upper = SPANS - 1 - owner
    first = jnp.where(flips == 1, upper, lower)
    second = jnp.where(flips == 1, lower, upper)
    return jnp.stack([first, second], axis=1).reshape(SPANS).astype(jnp.int32)


def steps_of(stream_key, extent, pieces, low, high):
    def one(axis_at, shards_of):
        draws = jax.random.uniform(jax.random.fold_in(jax.random.fold_in(stream_key, 6), axis_at), (shards_of,), jnp.float32, low / len(pieces), high / len(pieces))
        return jnp.repeat(jnp.exp(draws), extent[axis_at] // shards_of).reshape((-1,) + (1,) * (len(extent) - axis_at - 1))

    factor_of = one(*pieces[0])
    for cut in pieces[1:]:
        factor_of = factor_of * one(*cut)
    return factor_of


def noise(own_key, extent, width, limit, cuts=(), held_as=jnp.bfloat16):
    level = steps_of(own_key, extent, cuts, -0.22, 0.18) if cuts else 1.0
    values = jax.random.normal(own_key, extent, jnp.float32) * width * level
    return jnp.minimum(jnp.maximum(values, -limit), limit).astype(held_as)


def setup_inputs(seed: int = 0, part: int = 0) -> dict:
    key_list = jax.random.split(jax.random.key(seed), 5)
    own_keys = jax.random.split(jax.random.fold_in(key_list[4], part), 5)
    queries = draw_queries(jax.random.fold_in(jax.random.fold_in(key_list[4], part), 71), part)
    keys = draw_keys(jax.random.fold_in(jax.random.fold_in(key_list[4], part), 71), part)
    values = noise(own_keys[2], (TOKENS, KV_HEADS * HEAD), 1.0, 6.0, ((0, 16),))
    span_order = draw_span_order(jax.random.fold_in(jax.random.fold_in(key_list[4], part), 71), part)
    return dict(queries=queries, keys=keys, values=values, span_order=span_order)


def reference(queries, keys, values, span_order):
    span = TOK_DEV // 2
    group = HEADS // KV_HEADS
    rows = jnp.arange(TOKENS, dtype=jnp.int32)
    position = (span_order[rows // span] * span + rows % span).astype(jnp.int32)
    qall = queries.astype(jnp.float32).reshape(TOKENS, KV_HEADS, group, HEAD)
    kall = keys.astype(jnp.float32).reshape(TOKENS, KV_HEADS, HEAD)
    vall = values.astype(jnp.float32).reshape(TOKENS, KV_HEADS, HEAD)
    scale = 1.0 / (HEAD ** 0.5)
    block = 128
    count = TOKENS // block

    def one_block(index):
        start = (index * block).astype(jnp.int32)
        qblock = lax.dynamic_slice_in_dim(qall, start, block, 0)
        pblock = lax.dynamic_slice_in_dim(position, start, block, 0)
        scores = jnp.einsum('rkgd,ckd->kgrc', qblock, kall) * scale
        scores = jnp.where(position[None, None, None, :] <= pblock[None, None, :, None], scores, -jnp.inf)
        top = jnp.max(scores, axis=-1, keepdims=True)
        expo = jnp.exp(scores - top)
        total = jnp.sum(expo, axis=-1)
        weights = expo.astype(jnp.bfloat16).astype(jnp.float32)
        summed = jnp.einsum('kgrc,ckd->kgrd', weights, vall) / total[..., None]
        return summed.transpose(2, 0, 1, 3).reshape(block, HEADS * HEAD).astype(jnp.bfloat16)

    result = lax.map(one_block, jnp.arange(count, dtype=jnp.int32))
    return result.reshape(TOKENS, HEADS * HEAD)
```

```python
import functools
import math

import jax
import jax.numpy as jnp
from jax import lax
from jax.experimental import pallas as pl
from jax.experimental.pallas import tpu as pltpu
from jax.sharding import PartitionSpec as P

HEAD = 128
CORES = 2
TILE_SPANS = 8


def chip_at(place, chips):
    half = chips // 2
    return 2 * place if place < half else 2 * (chips - 1 - place) + 1


def place_of(chip, chips):
    return chip // 2 if chip % 2 == 0 else chips - 1 - chip // 2


def way(core, step):
    return 1 if (core + step) % 2 == 0 else -1


def ring_pairs(size, step):
    chips = size // CORES
    pairs = []
    for device in range(size):
        chip, core = device // CORES, device % CORES
        place = (place_of(chip, chips) + way(core, step)) % chips
        pairs.append((device, chip_at(place, chips) * CORES + 1 - core))
    return pairs


def mate_pairs(size):
    return [(device, device ^ 1) for device in range(size)]


def gather(rows_kv):
    size = lax.axis_size("blk")
    chips = size // CORES
    rows = rows_kv.shape[0]
    swap = functools.partial(lax.ppermute, axis_name="blk", perm=mate_pairs(size))
    unit = jnp.concatenate([rows_kv, swap(rows_kv)], axis=0)
    pieces = [(unit, 0, True)]
    for step in range(1, chips // 2 + 1):
        if step == chips // 2:
            unit = unit[:rows]
        unit = lax.ppermute(unit, "blk", ring_pairs(size, step))
        pieces.append((unit, step, True))
        pieces.append((swap(unit), step, False))
    return pieces


def attend_kernel(plan, rows, group, kv_heads, count, q_ref, order_ref, *refs):
    piece_refs = refs[: len(plan)]
    out_ref = refs[len(plan)]
    held = refs[len(plan) + 1]
    span = rows // 2
    tile = TILE_SPANS * span
    tiles = count // tile
    chips = lax.axis_size("blk") // CORES
    half = chips // 2
    mine = lax.axis_index("blk")
    core = mine % CORES
    chip = mine // CORES
    place = jnp.where(chip % 2 == 0, chip // 2, chips - 1 - chip // 2)
    for ref, (step, own) in zip(piece_refs, plan):
        holder = core if own else 1 - core
        direction = 1 - 2 * ((1 - holder + step) % 2)
        spot = (place + chips - direction * step) % chips
        from_chip = jnp.where(spot < half, 2 * spot, 2 * (chips - 1 - spot) + 1)
        first = (holder + step) % 2
        for part in range(ref.shape[0] // rows):
            device = from_chip * CORES + (first if part == 0 else 1 - first)
            for slot in range(2):
                target = order_ref[device * 2 + slot] * span
                held[pl.ds(pl.multiple_of(target, span), span), :] = ref[
                    pl.ds(part * rows + slot * span, span), :
                ]
    slot_pos = (order_ref[mine * 2], order_ref[mine * 2 + 1])
    low_slot = jnp.where(slot_pos[0] < slot_pos[1], 0, 1)
    low_pos = jnp.minimum(slot_pos[0], slot_pos[1])
    high_pos = jnp.maximum(slot_pos[0], slot_pos[1])
    low_row = pl.multiple_of(low_slot * span, span)
    high_row = pl.multiple_of((1 - low_slot) * span, span)
    scale = math.log2(math.e) / HEAD**0.5
    gap = lax.broadcasted_iota(jnp.int32, (span, tile), 1) - lax.broadcasted_iota(
        jnp.int32, (span, tile), 0
    )
    width = kv_heads * HEAD

    def rows_of(start, kv_head):
        parts = [
            q_ref[pl.ds(start, span), (kv_head * group + g) * HEAD : (kv_head * group + g + 1) * HEAD]
            for g in range(group)
        ]
        return jnp.concatenate(parts, axis=0)

    def scores(query, kv_head, key_tile, limit):
        start = key_tile * tile
        if not isinstance(start, int):
            start = pl.multiple_of(start, tile)
        keys = held[pl.ds(start, tile), kv_head * HEAD : (kv_head + 1) * HEAD]
        raw = lax.dot_general(
            query, keys, (((1,), (1,)), ((), ())), preferred_element_type=jnp.float32
        )
        if limit is None:
            return raw
        keep = gap <= limit * span - start
        shaped = raw.reshape(group, span, tile)
        return jnp.where(keep[None], shaped, -jnp.inf).reshape(group * span, tile)

    def weighted(expo, kv_head, key_tile):
        start = key_tile * tile
        if not isinstance(start, int):
            start = pl.multiple_of(start, tile)
        rows_v = held[pl.ds(start, tile), width + kv_head * HEAD : width + (kv_head + 1) * HEAD]
        return jnp.dot(expo.astype(jnp.bfloat16), rows_v, preferred_element_type=jnp.float32)

    def top(items):
        return jnp.max(functools.reduce(jnp.maximum, items), axis=-1, keepdims=True)

    reach = low_pos // TILE_SPANS
    middle = tiles // 2
    for kv_head in range(kv_heads):
        high_q = rows_of(high_row, kv_head)
        low_q = rows_of(low_row, kv_head)
        high_s = [
            scores(high_q, kv_head, t, high_pos if t == middle else None) for t in range(middle + 1)
        ]
        low_s = scores(low_q, kv_head, 0, low_pos)
        high_m = top(high_s)
        low_m = top([low_s])
        extra = []
        for j in range(1, middle):
            is_low = reach >= j
            row = pl.multiple_of(jnp.where(is_low, low_row, high_row), span)
            key_tile = jnp.where(is_low, j, tiles - j)
            s = scores(
                rows_of(row, kv_head), kv_head, key_tile, jnp.where(is_low, low_pos, high_pos)
            )
            m = top([s])
            low_m = jnp.where(is_low, jnp.maximum(low_m, m), low_m)
            high_m = jnp.where(is_low, high_m, jnp.maximum(high_m, m))
            extra.append((s, is_low, key_tile))

        def expo_of(s, m):
            return jnp.exp2((s - m) * scale)

        high_l = low_l = 0.0
        high_o = low_o = 0.0
        for t, s in enumerate(high_s):
            e = expo_of(s, high_m)
            high_l = high_l + jnp.sum(e, axis=-1, keepdims=True)
            high_o = high_o + weighted(e, kv_head, t)
        e = expo_of(low_s, low_m)
        low_l = low_l + jnp.sum(e, axis=-1, keepdims=True)
        low_o = low_o + weighted(e, kv_head, 0)
        for s, is_low, key_tile in extra:
            e = expo_of(s, jnp.where(is_low, low_m, high_m))
            l = jnp.sum(e, axis=-1, keepdims=True)
            o = weighted(e, kv_head, key_tile)
            low_l = low_l + jnp.where(is_low, l, 0.0)
            high_l = high_l + jnp.where(is_low, 0.0, l)
            low_o = low_o + jnp.where(is_low, o, 0.0)
            high_o = high_o + jnp.where(is_low, 0.0, o)
        for start, o, l in ((high_row, high_o, high_l), (low_row, low_o, low_l)):
            normed = (o / l).astype(jnp.bfloat16)
            for g in range(group):
                out_ref[
                    pl.ds(start, span),
                    (kv_head * group + g) * HEAD : (kv_head * group + g + 1) * HEAD,
                ] = normed[g * span : (g + 1) * span]


def per_device(queries, keys, values, span_order):
    rows = queries.shape[0]
    kv_heads = keys.shape[1] // HEAD
    group = queries.shape[1] // (kv_heads * HEAD)
    count = rows * lax.axis_size("blk")
    pieces = gather(jnp.concatenate([keys, values], axis=1))
    plan = [(step, own) for _, step, own in pieces]
    vmem = pl.BlockSpec(memory_space=pltpu.VMEM)
    return pl.pallas_call(
        functools.partial(attend_kernel, plan, rows, group, kv_heads, count),
        out_shape=jax.ShapeDtypeStruct(queries.shape, jnp.bfloat16),
        in_specs=[vmem, pl.BlockSpec(memory_space=pltpu.SMEM)] + [vmem] * len(pieces),
        out_specs=vmem,
        scratch_shapes=[pltpu.VMEM((count, 2 * kv_heads * HEAD), jnp.bfloat16)],
    )(queries, span_order, *[array for array, _, _ in pieces])


def solution(mesh):
    return jax.shard_map(
        per_device,
        mesh=mesh,
        in_specs=(
            P(("parts", "blk"), None),
            P(("parts", "blk"), None),
            P(("parts", "blk"), None),
            P("parts"),
        ),
        out_specs=P(("parts", "blk"), None),
        check_vma=False,
    )
```

```python
import functools
import math

import jax
import jax.numpy as jnp
from jax import lax
from jax.experimental import pallas as pl
from jax.experimental.pallas import tpu as pltpu
from jax.sharding import PartitionSpec as P


HEAD = 128
CORES = 2
TILE_SPANS = 8
LANES = 128
SCALE = math.log2(math.e) / HEAD**0.5


def chip_at(place, chips):
    half = chips // 2
    return 2 * place if place < half else 2 * (chips - 1 - place) + 1


def place_of(chip, chips):
    return chip // 2 if chip % 2 == 0 else chips - 1 - chip // 2


def ring_pairs(size, sender, receiver, hops):
    chips = size // CORES
    pairs = []
    for device in range(size):
        chip, core = device // CORES, device % CORES
        ahead = core == sender
        place = (place_of(chip, chips) + (hops if ahead else -hops)) % chips
        target = receiver if ahead else 1 - receiver
        pairs.append((device, chip_at(place, chips) * CORES + target))
    return pairs


def mate_pairs(size):
    return [(device, device ^ 1) for device in range(size)]


def gather(mine):
    size = lax.axis_size("blk")
    far = size // CORES // 2

    def swap(array):
        return lax.ppermute(array, "blk", mate_pairs(size))

    def send(array, sender, receiver, hops):
        return lax.ppermute(array, "blk", ring_pairs(size, sender, receiver, hops))

    mate = swap(mine)
    pieces = [(mine, 0, 0, 0, True), (mate, 0, 0, 0, False)]
    lead = follow = None
    held = 0
    for step in range(1, far + 1):
        for rest in range(2 if step < far else 1):
            source = (mate if rest else mine) if step == 1 else (follow if rest else lead)
            got = send(source, held, 1 - held, 1)
            if rest:
                follow = got
            else:
                lead = got
            pieces.append((got, step, 1 - held, rest, True))
            pieces.append((swap(got), step, 1 - held, rest, False))
        held = 1 - held
    return pieces


def ring_spot(size):
    chips = size // CORES
    mine = lax.axis_index("blk")
    chip = mine // CORES
    place = jnp.where(chip % 2 == 0, chip // 2, chips - 1 - chip // 2)
    return mine, chip, mine % CORES, place, chips


def device_of(entry):
    distance, behind, rest, own = entry
    _, chip, core, place, chips = ring_spot(lax.axis_size("blk"))
    half = chips // 2
    holder = core if own else 1 - core
    if distance == 0:
        return chip * CORES + holder
    from_behind = (holder == behind).astype(jnp.int32)
    spot = (place + chips + distance - 2 * distance * from_behind) % chips
    from_chip = jnp.where(spot < half, 2 * spot, 2 * (chips - 1 - spot) + 1)
    return from_chip * CORES + rest + (1 - 2 * rest) * (1 - from_behind)


def blocks_of(piece, table):
    return [table[at // LANES, at % LANES] for at in (2 * piece, 2 * piece + 1)]


def own_blocks(table):
    first, second = blocks_of(0, table)
    in_order = first < second
    return in_order, jnp.minimum(first, second), jnp.maximum(first, second)


def setup_kernel(plan, order_ref, table):
    rows = table.shape[0]
    at = lax.broadcasted_iota(jnp.int32, (rows, LANES), 0) * LANES + lax.broadcasted_iota(
        jnp.int32, (rows, LANES), 1
    )
    wanted = jnp.zeros((rows, LANES), jnp.int32)
    for number, entry in enumerate(plan):
        device = device_of(entry)
        for slot in range(2):
            wanted = jnp.where(at == 2 * number + slot, device * 2 + slot, wanted)
    known = jnp.zeros((rows, LANES), jnp.int32)
    for block in range(order_ref.shape[1]):
        known = jnp.where(wanted == block, order_ref[0, block], known)
    table[...] = known


def load_kernel(table, q_ref, q_out, table_out):
    q_out[...] = q_ref[...]
    table_out[...] = table[...]


def place_kernel(numbers, missing, span, table, *refs):
    held = refs[-1]
    for number in missing:
        for block in blocks_of(number, table):
            at = pl.ds(pl.multiple_of(block * span, span), span)
            held[:, at, :] = jnp.zeros((held.shape[0], span, HEAD), held.dtype)
    for number, ref in zip(numbers, refs):
        for slot, block in enumerate(blocks_of(number, table)):
            at = pl.ds(pl.multiple_of(block * span, span), span)
            for part in range(held.shape[0]):
                held[part, at, :] = ref[
                    slot * span : (slot + 1) * span, part * HEAD : (part + 1) * HEAD
                ]


def place_first(numbers, missing, span, table, *refs):
    place_kernel(numbers, missing, span, table, *refs)


def place_aliased(numbers, missing, span, table, held_in, *refs):
    del held_in, missing
    place_kernel(numbers, [], span, table, *refs)


def head_columns(kv_head, g, group):
    return slice((kv_head * group + g) * HEAD, (kv_head * group + g + 1) * HEAD)


def query_rows(q_ref, span, kv_head, group, in_order):
    slots = [
        jnp.concatenate(
            [
                q_ref[slot * span : (slot + 1) * span, head_columns(kv_head, g, group)]
                for g in range(group)
            ],
            axis=0,
        )
        for slot in range(2)
    ]
    return jnp.where(in_order, slots[0], slots[1]), jnp.where(in_order, slots[1], slots[0])


def folded(array):
    parts = [array[:, at : at + HEAD] for at in range(0, array.shape[1], HEAD)]
    return functools.reduce(jnp.add, parts)


def attend_kernel(missing, kv_list, span, group, q_ref, table, held, sum_ref, top_ref, total_ref):
    kv_heads = held.shape[0] // 2
    tile = TILE_SPANS * span
    tiles = held.shape[1] // tile
    middle = tiles // 2
    in_order, low_pos, high_pos = own_blocks(table)
    absent = [block for number in missing for block in blocks_of(number, table)]
    gap = lax.broadcasted_iota(jnp.int32, (span, tile), 1) - lax.broadcasted_iota(
        jnp.int32, (span, tile), 0
    )
    lane_block = lax.broadcasted_iota(jnp.int32, (8, tile), 1) // span
    reach = low_pos // TILE_SPANS

    def bias_of(key_tile):
        block = lane_block + key_tile * TILE_SPANS
        gone = functools.reduce(jnp.logical_or, [block == b for b in absent])
        return jnp.where(gone, -jnp.inf, 0.0)

    def tile_of(part, key_tile):
        return held[part, key_tile * tile : (key_tile + 1) * tile, :]

    def scores(query, keys, key_tile, bias, limit):
        raw = lax.dot_general(
            query, keys, (((1,), (1,)), ((), ())), preferred_element_type=jnp.float32
        )
        raw = (raw.reshape(-1, 8, tile) + bias[None]).reshape(raw.shape)
        if limit is None:
            return raw
        keep = gap <= limit * span - key_tile * tile
        return jnp.where(keep[None], raw.reshape(-1, span, tile), -jnp.inf).reshape(raw.shape)

    def weighted(expo, rows_v):
        return jnp.dot(expo.astype(jnp.bfloat16), rows_v, preferred_element_type=jnp.float32)

    def top(items):
        return jnp.max(functools.reduce(jnp.maximum, items), axis=-1, keepdims=True)

    def expo_of(s, m):
        return jnp.exp2((s - m) * SCALE)

    extras = []
    for j in range(1, middle):
        is_low = reach >= j
        key_tile = jnp.where(is_low, j, tiles - j)
        limit = jnp.where(is_low, low_pos, high_pos)
        extras.append((j, is_low, key_tile, limit, bias_of(key_tile)))
    biases = [bias_of(t) for t in range(middle + 1)]
    for at, kv_head in enumerate(kv_list):
        low_q, high_q = query_rows(q_ref, span, kv_head, group, in_order)
        high_s = [
            scores(
                high_q, tile_of(kv_head, t), t, biases[t], high_pos if t == middle else None
            )
            for t in range(middle + 1)
        ]
        low_s = scores(low_q, tile_of(kv_head, 0), 0, biases[0], low_pos)
        high_m = top(high_s)
        low_m = top([low_s])
        extra_s = []
        for j, is_low, key_tile, limit, bias in extras:
            keys = jnp.where(is_low, tile_of(kv_head, j), tile_of(kv_head, tiles - j))
            s = scores(jnp.where(is_low, low_q, high_q), keys, key_tile, bias, limit)
            m = top([s])
            low_m = jnp.where(is_low, jnp.maximum(low_m, m), low_m)
            high_m = jnp.where(is_low, high_m, jnp.maximum(high_m, m))
            extra_s.append(s)
        high_l, high_o = 0.0, 0.0
        for t, s in enumerate(high_s):
            e = expo_of(s, high_m)
            high_l = high_l + folded(e)
            high_o = high_o + weighted(e, tile_of(kv_heads + kv_head, t))
        e = expo_of(low_s, low_m)
        low_l = folded(e)
        low_o = weighted(e, tile_of(kv_heads + kv_head, 0))
        for (j, is_low, key_tile, limit, bias), s in zip(extras, extra_s):
            e = expo_of(s, jnp.where(is_low, low_m, high_m))
            l = folded(e)
            v_part = kv_heads + kv_head
            o = weighted(e, jnp.where(is_low, tile_of(v_part, j), tile_of(v_part, tiles - j)))
            low_l = low_l + jnp.where(is_low, l, 0.0)
            high_l = high_l + jnp.where(is_low, 0.0, l)
            low_o = low_o + jnp.where(is_low, o, 0.0)
            high_o = high_o + jnp.where(is_low, 0.0, o)
        for side, (o, m, l) in enumerate(((low_o, low_m, low_l), (high_o, high_m, high_l))):
            sum_ref[at, side] = o
            top_ref[at, side] = jnp.broadcast_to(m, o.shape)
            total_ref[at, side] = l


def finish_kernel(plan, stages, span, group, kv_heads, q_ref, table, *refs):
    pieces = refs[: len(plan)]
    states = refs[len(plan) : len(plan) + 3 * len(stages)]
    out_ref, ready, sems = refs[len(plan) + 3 * len(stages) :]
    in_order, *positions = own_blocks(table)
    blocks = [block for number in plan for block in blocks_of(number, table)]
    keys = span * len(blocks)
    lane_block = lax.broadcasted_iota(jnp.int32, (8, keys), 1) // span
    position = functools.reduce(
        lambda held, item: jnp.where(lane_block == item[0], item[1], held),
        enumerate(blocks),
        jnp.zeros((8, keys), jnp.int32),
    )
    biases = [jnp.where(position < pos, 0.0, -jnp.inf) for pos in positions]
    width = kv_heads * HEAD

    def rows_of(column):
        return jnp.concatenate([ref[:, column : column + HEAD] for ref in pieces], axis=0)

    where = [(stage, at) for stage, kv_list in enumerate(stages) for at in range(len(kv_list))]
    tops, weights = [], []
    for kv_head, (stage, at) in enumerate(where):
        queries = query_rows(q_ref, span, kv_head, group, in_order)
        rows_k = rows_of(kv_head * HEAD)
        for side in range(2):
            s = lax.dot_general(
                queries[side], rows_k, (((1,), (1,)), ((), ())), preferred_element_type=jnp.float32
            )
            s = (s.reshape(-1, 8, keys) + biases[side][None]).reshape(s.shape)
            new_m = jnp.maximum(
                states[3 * stage + 1][at, side], jnp.max(s, axis=-1, keepdims=True)
            )
            tops.append(new_m)
            weights.append(jnp.exp2((s - new_m) * SCALE))
    copies = []
    for kv_head, (stage, at) in enumerate(where):
        rows_v = rows_of(width + kv_head * HEAD)
        normed = []
        for side in range(2):
            sum_ref, top_ref, total_ref = states[3 * stage : 3 * stage + 3]
            new_m, e = tops[2 * kv_head + side], weights[2 * kv_head + side]
            fade = jnp.exp2((top_ref[at, side] - new_m) * SCALE)
            l = jnp.sum(total_ref[at, side] * fade + folded(e), axis=-1, keepdims=True)
            o = sum_ref[at, side] * fade + jnp.dot(
                e.astype(jnp.bfloat16), rows_v, preferred_element_type=jnp.float32
            )
            normed.append((o / l).astype(jnp.bfloat16))
        low, high = normed
        for slot, rows in enumerate(
            (jnp.where(in_order, low, high), jnp.where(in_order, high, low))
        ):
            for g in range(group):
                ready[slot * span : (slot + 1) * span, head_columns(kv_head, g, group)] = rows[
                    g * span : (g + 1) * span
                ]
        columns = pl.ds(kv_head * group * HEAD, group * HEAD)
        copy = pltpu.make_async_copy(ready.at[:, columns], out_ref.at[:, columns], sems.at[kv_head])
        copy.start()
        copies.append(copy)
    for copy in copies:
        copy.wait()


def attended(queries, keys, values, span_order):
    rows = queries.shape[0]
    span = rows // 2
    kv_heads = keys.shape[1] // HEAD
    group = queries.shape[1] // (kv_heads * HEAD)
    size = lax.axis_size("blk")
    far = size // CORES // 2
    count = rows * size
    vmem = pl.BlockSpec(memory_space=pltpu.VMEM)
    anywhere = pl.BlockSpec(memory_space=pltpu.HBM)
    params = pltpu.CompilerParams(vmem_limit_bytes=8 * 2**20 + 6 * count * 2 * kv_heads * HEAD)

    def call(kernel, out_shape, in_specs, **extra):
        return pl.pallas_call(
            kernel, out_shape=out_shape, in_specs=in_specs, compiler_params=params, **extra
        )

    width = keys.shape[1]
    lowest = jnp.array(-jnp.inf, keys.dtype)
    mine = jnp.maximum(
        lax.pad(keys, lowest, ((0, 0, 0), (0, width, 0))),
        lax.pad(values, lowest, ((0, 0, 0), (width, 0, 0))),
    )
    pieces = gather(mine)
    plan = [p[1:] for p in pieces]
    table_rows = -(-2 * len(plan) // LANES)
    table = call(
        functools.partial(setup_kernel, plan),
        jax.ShapeDtypeStruct((table_rows, LANES), jnp.int32),
        [vmem],
        out_specs=vmem,
    )(span_order.reshape(1, -1))
    q_held, loaded = call(
        load_kernel,
        (
            jax.ShapeDtypeStruct(queries.shape, queries.dtype),
            jax.ShapeDtypeStruct(table.shape, table.dtype),
        ),
        [vmem, vmem],
        out_specs=(vmem, vmem),
    )(table, queries)
    missing = [number for number, entry in enumerate(plan) if entry[0] == far]
    last = [pieces[number] for number in missing]
    held_shape = jax.ShapeDtypeStruct((2 * kv_heads, count, HEAD), jnp.bfloat16)
    held = None
    placed = set(missing)
    for step in range(2, far + 1):
        numbers = []
        for number, entry in enumerate(plan):
            ready = step == far or entry[0] < step - 1 or (entry[0] == step - 1 and entry[3])
            if ready and number not in placed:
                numbers.append(number)
        placed.update(numbers)
        held = call(
            functools.partial(place_first if held is None else place_aliased, numbers, missing, span),
            held_shape,
            [vmem] * (len(numbers) + 1 + (held is not None)),
            out_specs=vmem,
            **({} if held is None else {"input_output_aliases": {1: 0}}),
        )(
            loaded if step == far else table,
            *([] if held is None else [held]),
            *[pieces[n][0] for n in numbers],
        )
    stages = [list(range(kv_heads // 2)), list(range(kv_heads // 2, kv_heads))]
    states = []
    for kv_list in stages:
        shape = jax.ShapeDtypeStruct((len(kv_list), 2, group * span, HEAD), jnp.float32)
        states += call(
            functools.partial(attend_kernel, missing, kv_list, span, group),
            (shape, shape, shape),
            [vmem, vmem, vmem],
            out_specs=(vmem, vmem, vmem),
        )(q_held, table, held)
    return call(
        functools.partial(finish_kernel, missing, stages, span, group, kv_heads),
        jax.ShapeDtypeStruct(queries.shape, jnp.bfloat16),
        [vmem] * (2 + len(last) + len(states)),
        out_specs=anywhere,
        scratch_shapes=[
            pltpu.VMEM(queries.shape, jnp.bfloat16),
            pltpu.SemaphoreType.DMA((kv_heads,)),
        ],
    )(q_held, table, *[p[0] for p in last], *states)


def solution(mesh):
    return jax.shard_map(
        attended,
        mesh=mesh,
        in_specs=(
            P(("parts", "blk"), None),
            P(("parts", "blk"), None),
            P(("parts", "blk"), None),
            P("parts"),
        ),
        out_specs=P(("parts", "blk"), None),
        check_vma=False,
    )
```

```python
import functools
import math

import jax
import jax.numpy as jnp
from jax import lax
from jax.experimental import pallas as pl
from jax.experimental.pallas import tpu as pltpu
from jax.sharding import PartitionSpec as P


HEAD = 128
CORES = 2
TILE_SPANS = 8
LANES = 128
CUTS = 2
SCALE = math.log2(math.e) / HEAD**0.5


def chip_at(place, chips):
    half = chips // 2
    return 2 * place if place < half else 2 * (chips - 1 - place) + 1


def place_of(chip, chips):
    return chip // 2 if chip % 2 == 0 else chips - 1 - chip // 2


def ring_pairs(size, sender, receiver, hops):
    chips = size // CORES
    pairs = []
    for device in range(size):
        chip, core = device // CORES, device % CORES
        ahead = core == sender
        place = (place_of(chip, chips) + (hops if ahead else -hops)) % chips
        target = receiver if ahead else 1 - receiver
        pairs.append((device, chip_at(place, chips) * CORES + target))
    return pairs


def mate_pairs(size):
    return [(device, device ^ 1) for device in range(size)]


def gather(mine):
    size = lax.axis_size("blk")
    far = size // CORES // 2

    def swap(array):
        return lax.ppermute(array, "blk", mate_pairs(size))

    def send(array, sender, receiver, hops):
        return lax.ppermute(array, "blk", ring_pairs(size, sender, receiver, hops))

    mate = swap(mine)
    pieces = [(mine, 0, 0, 0, True), (mate, 0, 0, 0, False)]
    lead = follow = None
    held = 0
    for step in range(1, far + 1):
        for rest in range(2 if step < far else 1):
            source = (mate if rest else mine) if step == 1 else (follow if rest else lead)
            got = send(source, held, 1 - held, 1)
            if rest:
                follow = got
            else:
                lead = got
            pieces.append((got, step, 1 - held, rest, True))
            pieces.append((swap(got), step, 1 - held, rest, False))
        held = 1 - held
    return pieces


def ring_spot(size):
    chips = size // CORES
    mine = lax.axis_index("blk")
    chip = mine // CORES
    place = jnp.where(chip % 2 == 0, chip // 2, chips - 1 - chip // 2)
    return mine, chip, mine % CORES, place, chips


def device_of(entry):
    distance, behind, rest, own = entry
    _, chip, core, place, chips = ring_spot(lax.axis_size("blk"))
    half = chips // 2
    holder = core if own else 1 - core
    if distance == 0:
        return chip * CORES + holder
    from_behind = (holder == behind).astype(jnp.int32)
    spot = (place + chips + distance - 2 * distance * from_behind) % chips
    from_chip = jnp.where(spot < half, 2 * spot, 2 * (chips - 1 - spot) + 1)
    return from_chip * CORES + rest + (1 - 2 * rest) * (1 - from_behind)


def blocks_of(piece, table):
    return [table[at // LANES, at % LANES] for at in (2 * piece, 2 * piece + 1)]


def own_blocks(table):
    first, second = blocks_of(0, table)
    in_order = first < second
    return in_order, jnp.minimum(first, second), jnp.maximum(first, second)


def setup_kernel(plan, order_ref, table):
    rows = table.shape[0]
    at = lax.broadcasted_iota(jnp.int32, (rows, LANES), 0) * LANES + lax.broadcasted_iota(
        jnp.int32, (rows, LANES), 1
    )
    wanted = jnp.zeros((rows, LANES), jnp.int32)
    for number, entry in enumerate(plan):
        device = device_of(entry)
        for slot in range(2):
            wanted = jnp.where(at == 2 * number + slot, device * 2 + slot, wanted)
    known = jnp.zeros((rows, LANES), jnp.int32)
    for block in range(order_ref.shape[1]):
        known = jnp.where(wanted == block, order_ref[0, block], known)
    table[...] = known


def load_kernel(table, q_ref, q_out, table_out):
    q_out[...] = q_ref[...]
    table_out[...] = table[...]


def put_block(held, block, span, rows, present):
    at = pl.ds(pl.multiple_of(block * span, span), span)
    parts = held.shape[0] - 1
    for part in range(parts):
        held[part, at, :] = rows(part)
    held[parts, at, :] = jnp.full((span, HEAD), present, held.dtype)


def place_kernel(numbers, span, table, pieces, held):
    for number, ref in zip(numbers, pieces):
        for slot, block in enumerate(blocks_of(number, table)):
            put_block(
                held,
                block,
                span,
                lambda part: ref[slot * span : (slot + 1) * span, part * HEAD : (part + 1) * HEAD],
                1.0,
            )


def place_first(numbers, missing, span, table, *refs):
    *pieces, held = refs
    mine = pieces[0]
    in_order, _, _ = own_blocks(table)
    keys = (held.shape[0] - 1) // 2

    def stand_in(part):
        if part >= keys:
            return jnp.zeros((span, HEAD), held.dtype)
        columns = slice(part * HEAD, (part + 1) * HEAD)
        both = [mine[slot * span : slot * span + 1, columns].astype(jnp.float32) for slot in range(2)]
        row = jnp.where(in_order, both[0], both[1])
        return jnp.broadcast_to(row, (span, HEAD)).astype(held.dtype)

    fills = [stand_in(part) for part in range(2 * keys)]
    for number in missing:
        for block in blocks_of(number, table):
            put_block(held, block, span, lambda part: fills[part], 0.0)
    place_kernel(numbers, span, table, pieces, held)


def place_more(numbers, span, table, held_in, *refs):
    del held_in
    *pieces, held = refs
    place_kernel(numbers, span, table, pieces, held)


def head_columns(kv_head, g, group):
    return slice((kv_head * group + g) * HEAD, (kv_head * group + g + 1) * HEAD)


def query_rows(q_ref, span, kv_head, group, in_order, heads):
    slots = [
        jnp.concatenate(
            [
                q_ref[slot * span : (slot + 1) * span, head_columns(kv_head, g, group)]
                for g in heads
            ],
            axis=0,
        )
        for slot in range(2)
    ]
    return jnp.where(in_order, slots[0], slots[1]), jnp.where(in_order, slots[1], slots[0])


def attend_kernel(kv_list, span, group, q_ref, table, held, sum_ref, top_ref, total_ref):
    kv_heads = (held.shape[0] - 1) // 2
    tile = TILE_SPANS * span
    tiles = held.shape[1] // tile
    middle = tiles // 2
    in_order, low_pos, high_pos = own_blocks(table)
    gap = lax.broadcasted_iota(jnp.int32, (span, tile), 1) - lax.broadcasted_iota(
        jnp.int32, (span, tile), 0
    )
    reach = low_pos // TILE_SPANS

    def masked(raw, key_tile, limit):
        keep = gap <= limit * span - key_tile * tile
        return jnp.where(keep[None], raw.reshape(-1, span, tile), -jnp.inf).reshape(raw.shape)

    def scores(query, keys):
        return lax.dot_general(
            query, keys, (((1,), (1,)), ((), ())), preferred_element_type=jnp.float32
        )

    def weighted(expo, rows_v):
        return jnp.dot(expo.astype(jnp.bfloat16), rows_v, preferred_element_type=jnp.float32)

    def top(items):
        return jnp.max(functools.reduce(jnp.maximum, items), axis=-1, keepdims=True)

    def expo_of(s, m):
        return jnp.exp2((s - m) * SCALE)

    def keys_at(kv_head, first, last):
        return held[kv_head, first * tile : last * tile, :]

    def values_at(kv_head, first, last):
        rows = slice(first * tile, last * tile)
        return jnp.concatenate([held[kv_heads + kv_head, rows, :], held[2 * kv_heads, rows, :]], 1)

    extras = []
    for j in range(1, middle):
        is_low = reach >= j
        extras.append(
            (j, is_low, jnp.where(is_low, j, tiles - j), jnp.where(is_low, low_pos, high_pos))
        )

    def score_all(kv_head, heads):
        low_q, high_q = query_rows(q_ref, span, kv_head, group, in_order, heads)
        full_s = scores(high_q, keys_at(kv_head, 0, middle + 1))
        high_s = [full_s[:, t * tile : (t + 1) * tile] for t in range(middle + 1)]
        high_s[middle] = masked(high_s[middle], middle, high_pos)
        low_s = masked(scores(low_q, keys_at(kv_head, 0, 1)), 0, low_pos)
        high_m = top(high_s)
        low_m = top([low_s])
        extra_s = []
        for j, is_low, key_tile, limit in extras:
            keys = jnp.where(
                is_low, keys_at(kv_head, j, j + 1), keys_at(kv_head, tiles - j, tiles - j + 1)
            )
            s = masked(scores(jnp.where(is_low, low_q, high_q), keys), key_tile, limit)
            m = top([s])
            low_m = jnp.where(is_low, jnp.maximum(low_m, m), low_m)
            high_m = jnp.where(is_low, high_m, jnp.maximum(high_m, m))
            extra_s.append(s)
        return high_s, low_s, extra_s, high_m, low_m

    def weigh(at, kv_head, heads, high_s, low_s, extra_s, high_m, low_m):
        high_o = weighted(
            jnp.concatenate([expo_of(s, high_m) for s in high_s], axis=1),
            values_at(kv_head, 0, middle + 1),
        )
        low_o = weighted(expo_of(low_s, low_m), values_at(kv_head, 0, 1))
        for (j, is_low, _, _), s in zip(extras, extra_s):
            rows_v = jnp.where(
                is_low, values_at(kv_head, j, j + 1), values_at(kv_head, tiles - j, tiles - j + 1)
            )
            o = weighted(expo_of(s, jnp.where(is_low, low_m, high_m)), rows_v)
            low_o = low_o + jnp.where(is_low, o, 0.0)
            high_o = high_o + jnp.where(is_low, 0.0, o)
        for side, (o, m) in enumerate(((low_o, low_m), (high_o, high_m))):
            out = slice(heads[0] * span, (heads[-1] + 1) * span)
            sum_ref[at, side, out] = o[:, :HEAD]
            total_ref[at, side, out] = o[:, HEAD:]
            top_ref[at, side, out] = jnp.broadcast_to(m, (o.shape[0], HEAD))

    cuts = max(1, CUTS - len(kv_list) + 1)
    many = -(-group // cuts)
    units = [
        (at, kv_head, range(first, min(group, first + many)))
        for at, kv_head in enumerate(kv_list)
        for first in range(0, group, many)
    ]
    scored = [score_all(kv_head, heads) for _, kv_head, heads in units]
    for unit, found in zip(units, scored):
        weigh(*unit, *found)


def finish_kernel(numbers, lacks, stages, span, group, kv_heads, q_ref, table, *refs):
    pieces = dict(zip(numbers, refs))
    states = refs[len(numbers) : len(numbers) + 3 * len(stages)]
    out_ref, ready, sems = refs[len(numbers) + 3 * len(stages) :]
    in_order, *positions = own_blocks(table)
    width = kv_heads * HEAD
    biases = []
    for lack in lacks:
        blocks = [block for number in lack for block in blocks_of(number, table)]
        lane_block = lax.broadcasted_iota(jnp.int32, (8, span * len(blocks)), 1) // span
        position = jnp.zeros(lane_block.shape, jnp.int32)
        for number, block in enumerate(blocks):
            position = jnp.where(lane_block == number, block, position)
        biases.append([jnp.where(position < pos, 0.0, -jnp.inf) for pos in positions])

    def rows_of(stage, column):
        parts = [pieces[number][:, column : column + HEAD] for number in lacks[stage]]
        return jnp.concatenate(parts, axis=0)

    where = [(stage, at) for stage, kv_list in enumerate(stages) for at in range(len(kv_list))]
    copies = []
    for kv_head, (stage, at) in enumerate(where):
        sum_ref, top_ref, total_ref = states[3 * stage : 3 * stage + 3]
        queries = query_rows(q_ref, span, kv_head, group, in_order, range(group))
        rows_k = rows_of(stage, kv_head * HEAD)
        rows_v = rows_of(stage, width + kv_head * HEAD)
        rows_v = jnp.concatenate([rows_v, jnp.ones(rows_v.shape, rows_v.dtype)], axis=1)
        normed = []
        for side in range(2):
            s = lax.dot_general(
                queries[side], rows_k, (((1,), (1,)), ((), ())), preferred_element_type=jnp.float32
            )
            s = (s.reshape(-1, 8, s.shape[1]) + biases[stage][side][None]).reshape(s.shape)
            m = top_ref[at, side]
            new_m = jnp.maximum(m, jnp.max(s, axis=-1, keepdims=True))
            wide = jnp.concatenate([new_m] * (s.shape[1] // HEAD), axis=1)
            e = jnp.exp2((s - wide) * SCALE).astype(jnp.bfloat16)
            fade = jnp.exp2((m - new_m) * SCALE)
            more = jnp.dot(e, rows_v, preferred_element_type=jnp.float32)
            o = sum_ref[at, side] * fade + more[:, :HEAD]
            l = total_ref[at, side] * fade + more[:, HEAD:]
            normed.append((o / l).astype(jnp.bfloat16))
        low, high = normed
        for slot, rows in enumerate(
            (jnp.where(in_order, low, high), jnp.where(in_order, high, low))
        ):
            for g in range(group):
                ready[slot * span : (slot + 1) * span, head_columns(kv_head, g, group)] = rows[
                    g * span : (g + 1) * span
                ]
        columns = pl.ds(kv_head * group * HEAD, group * HEAD)
        copy = pltpu.make_async_copy(ready.at[:, columns], out_ref.at[:, columns], sems.at[kv_head])
        copy.start()
        copies.append(copy)
    for copy in copies:
        copy.wait()


def attended(queries, keys, values, span_order):
    rows = queries.shape[0]
    span = rows // 2
    kv_heads = keys.shape[1] // HEAD
    group = queries.shape[1] // (kv_heads * HEAD)
    size = lax.axis_size("blk")
    far = size // CORES // 2
    count = rows * size
    vmem = pl.BlockSpec(memory_space=pltpu.VMEM)
    anywhere = pl.BlockSpec(memory_space=pltpu.HBM)
    params = pltpu.CompilerParams(vmem_limit_bytes=8 * 2**20 + 6 * count * 2 * kv_heads * HEAD)

    def call(kernel, out_shape, in_specs, **extra):
        return pl.pallas_call(
            kernel, out_shape=out_shape, in_specs=in_specs, compiler_params=params, **extra
        )

    width = keys.shape[1]
    lowest = jnp.array(-jnp.inf, keys.dtype)
    mine = jnp.maximum(
        lax.pad(keys, lowest, ((0, 0, 0), (0, width, 0))),
        lax.pad(values, lowest, ((0, 0, 0), (width, 0, 0))),
    )
    pieces = gather(mine)
    plan = [p[1:] for p in pieces]
    table_rows = -(-2 * len(plan) // LANES)
    table = call(
        functools.partial(setup_kernel, plan),
        jax.ShapeDtypeStruct((table_rows, LANES), jnp.int32),
        [vmem],
        out_specs=vmem,
    )(span_order.reshape(1, -1))
    q_held, loaded = call(
        load_kernel,
        (
            jax.ShapeDtypeStruct(queries.shape, queries.dtype),
            jax.ShapeDtypeStruct(table.shape, table.dtype),
        ),
        [vmem, vmem],
        out_specs=(vmem, vmem),
    )(table, queries)
    lacks = [
        [n for n, e in enumerate(plan) if e[0] == far or (e[0] == far - 1 and not e[3])],
        [n for n, e in enumerate(plan) if e[0] == far],
    ]
    stages = [list(range(kv_heads - 1)), list(range(kv_heads - 1, kv_heads))]
    held_shape = jax.ShapeDtypeStruct((2 * kv_heads + 1, count, HEAD), jnp.bfloat16)
    held = None
    states = []

    def place(numbers, held, source):
        kernel = (
            functools.partial(place_first, numbers, lacks[0], span)
            if held is None
            else functools.partial(place_more, numbers, span)
        )
        before = [] if held is None else [held]
        extra = {} if held is None else {"input_output_aliases": {1: 0}}
        return call(
            kernel, held_shape, [vmem] * (1 + len(before) + len(numbers)), out_specs=vmem, **extra
        )(source, *before, *[pieces[number][0] for number in numbers])

    def attend(stage, held):
        shape = jax.ShapeDtypeStruct((len(stages[stage]), 2, group * span, HEAD), jnp.float32)
        return call(
            functools.partial(attend_kernel, stages[stage], span, group),
            (shape, shape, shape),
            [vmem, vmem, vmem],
            out_specs=(vmem, vmem, vmem),
        )(q_held, table, held)

    placed = set(lacks[0])
    for step in range(2, far + 1):
        numbers = []
        for number, entry in enumerate(plan):
            ready = step == far or entry[0] < step - 1 or (entry[0] == step - 1 and entry[3])
            if ready and number not in placed:
                numbers.append(number)
        placed.update(numbers)
        held = place(numbers, held, loaded if step == far else table)
    states += attend(0, held)
    rest = [number for number in lacks[0] if number not in lacks[1]]
    held = place(rest, held, table)
    states += attend(1, held)
    numbers = lacks[0]
    return call(
        functools.partial(finish_kernel, numbers, lacks, stages, span, group, kv_heads),
        jax.ShapeDtypeStruct(queries.shape, jnp.bfloat16),
        [vmem] * (2 + len(numbers) + len(states)),
        out_specs=anywhere,
        scratch_shapes=[
            pltpu.VMEM(queries.shape, jnp.bfloat16),
            pltpu.SemaphoreType.DMA((kv_heads,)),
        ],
    )(q_held, table, *[pieces[number][0] for number in numbers], *states)


def solution(mesh):
    return jax.shard_map(
        attended,
        mesh=mesh,
        in_specs=(
            P(("parts", "blk"), None),
            P(("parts", "blk"), None),
            P(("parts", "blk"), None),
            P("parts"),
        ),
        out_specs=P(("parts", "blk"), None),
        check_vma=False,
    )
```

```python
import functools
import math

import jax
import jax.numpy as jnp
from jax import lax
from jax.experimental import pallas as pl
from jax.experimental.pallas import tpu as pltpu
from jax.sharding import PartitionSpec as P


HEAD = 128
CORES = 2
TILE_SPANS = 8
LANES = 128
CUTS = 2
SCALE = math.log2(math.e) / HEAD**0.5


def chip_at(place, chips):
    half = chips // 2
    return 2 * place if place < half else 2 * (chips - 1 - place) + 1


def place_of(chip, chips):
    return chip // 2 if chip % 2 == 0 else chips - 1 - chip // 2


def ring_pairs(size, sender, receiver, hops):
    chips = size // CORES
    pairs = []
    for device in range(size):
        chip, core = device // CORES, device % CORES
        ahead = core == sender
        place = (place_of(chip, chips) + (hops if ahead else -hops)) % chips
        target = receiver if ahead else 1 - receiver
        pairs.append((device, chip_at(place, chips) * CORES + target))
    return pairs


def mate_pairs(size):
    return [(device, device ^ 1) for device in range(size)]


def gather(mine):
    size = lax.axis_size("blk")
    far = size // CORES // 2

    def swap(array):
        return lax.ppermute(array, "blk", mate_pairs(size))

    def send(array, sender, receiver, hops):
        return lax.ppermute(array, "blk", ring_pairs(size, sender, receiver, hops))

    mate = swap(mine)
    pieces = [(mine, 0, 0, 0, True), (mate, 0, 0, 0, False)]
    lead = follow = None
    held = 0
    for step in range(1, far + 1):
        for rest in range(2 if step < far else 1):
            source = (mate if rest else mine) if step == 1 else (follow if rest else lead)
            got = send(source, held, 1 - held, 1)
            if rest:
                follow = got
            else:
                lead = got
            pieces.append((got, step, 1 - held, rest, True))
            pieces.append((swap(got), step, 1 - held, rest, False))
        held = 1 - held
    return pieces


def ring_spot(size):
    chips = size // CORES
    mine = lax.axis_index("blk")
    chip = mine // CORES
    place = jnp.where(chip % 2 == 0, chip // 2, chips - 1 - chip // 2)
    return mine, chip, mine % CORES, place, chips


def device_of(entry):
    distance, behind, rest, own = entry
    _, chip, core, place, chips = ring_spot(lax.axis_size("blk"))
    half = chips // 2
    holder = core if own else 1 - core
    if distance == 0:
        return chip * CORES + holder
    from_behind = (holder == behind).astype(jnp.int32)
    spot = (place + chips + distance - 2 * distance * from_behind) % chips
    from_chip = jnp.where(spot < half, 2 * spot, 2 * (chips - 1 - spot) + 1)
    return from_chip * CORES + rest + (1 - 2 * rest) * (1 - from_behind)


def blocks_of(piece, table):
    return [table[at // LANES, at % LANES] for at in (2 * piece, 2 * piece + 1)]


def own_blocks(table):
    first, second = blocks_of(0, table)
    in_order = first < second
    return in_order, jnp.minimum(first, second), jnp.maximum(first, second)


def setup_kernel(plan, order_ref, table):
    rows = table.shape[0]
    at = lax.broadcasted_iota(jnp.int32, (rows, LANES), 0) * LANES + lax.broadcasted_iota(
        jnp.int32, (rows, LANES), 1
    )
    wanted = jnp.zeros((rows, LANES), jnp.int32)
    for number, entry in enumerate(plan):
        device = device_of(entry)
        for slot in range(2):
            wanted = jnp.where(at == 2 * number + slot, device * 2 + slot, wanted)
    known = jnp.zeros((rows, LANES), jnp.int32)
    for block in range(order_ref.shape[1]):
        known = jnp.where(wanted == block, order_ref[0, block], known)
    table[...] = known


def place_last(numbers, early, span, table, held_in, *refs):
    del held_in
    *pieces, held, tail = refs
    by_number = dict(zip(early, pieces))
    place_kernel(numbers, span, table, [by_number[number] for number in numbers], held)
    for spot, number in enumerate(early):
        first, second = blocks_of(number, table)
        ref = by_number[number]
        for slot, side in enumerate((first > second, first < second)):
            for part in range(tail.shape[0]):
                tail[part, side.astype(jnp.int32), spot * span : (spot + 1) * span, :] = ref[
                    slot * span : (slot + 1) * span, part * HEAD : (part + 1) * HEAD
                ]


def load_kernel(span, group, table, q_ref, q_out):
    in_order, _, _ = own_blocks(table)
    for kv_head in range(q_out.shape[0]):
        for g in range(group):
            columns = head_columns(kv_head, g, group)
            slots = [q_ref[slot * span : (slot + 1) * span, columns] for slot in range(2)]
            rows = slice(g * span, (g + 1) * span)
            q_out[kv_head, 0, rows, :] = jnp.where(in_order, slots[0], slots[1])
            q_out[kv_head, 1, rows, :] = jnp.where(in_order, slots[1], slots[0])


def put_block(held, block, span, rows, present):
    at = pl.ds(pl.multiple_of(block * span, span), span)
    parts = held.shape[0] - 1
    for part in range(parts):
        held[part, at, :] = rows(part)
    held[parts, at, :] = jnp.full((span, HEAD), present, held.dtype)


def place_kernel(numbers, span, table, pieces, held):
    for number, ref in zip(numbers, pieces):
        for slot, block in enumerate(blocks_of(number, table)):
            put_block(
                held,
                block,
                span,
                lambda part: ref[slot * span : (slot + 1) * span, part * HEAD : (part + 1) * HEAD],
                1.0,
            )


def place_first(numbers, missing, span, table, *refs):
    *pieces, held = refs
    mine = pieces[0]
    in_order, _, _ = own_blocks(table)
    keys = (held.shape[0] - 1) // 2

    def stand_in(part):
        if part >= keys:
            return jnp.zeros((span, HEAD), held.dtype)
        columns = slice(part * HEAD, (part + 1) * HEAD)
        both = [mine[slot * span : slot * span + 1, columns].astype(jnp.float32) for slot in range(2)]
        row = jnp.where(in_order, both[0], both[1])
        return jnp.broadcast_to(row, (span, HEAD)).astype(held.dtype)

    fills = [stand_in(part) for part in range(2 * keys)]
    for number in missing:
        for block in blocks_of(number, table):
            put_block(held, block, span, lambda part: fills[part], 0.0)
    place_kernel(numbers, span, table, pieces, held)


def place_more(numbers, span, table, held_in, *refs):
    del held_in
    *pieces, held = refs
    place_kernel(numbers, span, table, pieces, held)


def head_columns(kv_head, g, group):
    return slice((kv_head * group + g) * HEAD, (kv_head * group + g + 1) * HEAD)


def attend_kernel(kv_list, span, group, q_ref, table, held, sum_ref, top_ref, total_ref):
    kv_heads = (held.shape[0] - 1) // 2
    tile = TILE_SPANS * span
    tiles = held.shape[1] // tile
    middle = tiles // 2
    _, low_pos, high_pos = own_blocks(table)
    gap = lax.broadcasted_iota(jnp.int32, (span, tile), 1) - lax.broadcasted_iota(
        jnp.int32, (span, tile), 0
    )
    reach = low_pos // TILE_SPANS

    def masked(raw, key_tile, limit):
        keep = gap <= limit * span - key_tile * tile
        return jnp.where(keep[None], raw.reshape(-1, span, tile), -jnp.inf).reshape(raw.shape)

    def scores(query, keys):
        return lax.dot_general(
            query, keys, (((1,), (1,)), ((), ())), preferred_element_type=jnp.float32
        )

    def weighted(expo, rows_v):
        return jnp.dot(expo.astype(jnp.bfloat16), rows_v, preferred_element_type=jnp.float32)

    def top(items):
        return jnp.max(functools.reduce(jnp.maximum, items), axis=-1, keepdims=True)

    def expo_of(s, m):
        return jnp.exp2((s - m) * SCALE)

    def keys_at(kv_head, first, last):
        return held[kv_head, first * tile : last * tile, :]

    def values_at(kv_head, first, last):
        rows = slice(first * tile, last * tile)
        return jnp.concatenate([held[kv_heads + kv_head, rows, :], held[2 * kv_heads, rows, :]], 1)

    extras = []
    for j in range(1, middle):
        is_low = reach >= j
        extras.append(
            (j, is_low, jnp.where(is_low, j, tiles - j), jnp.where(is_low, low_pos, high_pos))
        )

    def score_all(kv_head, heads):
        rows = slice(heads[0] * span, (heads[-1] + 1) * span)
        low_q, high_q = q_ref[kv_head, 0, rows, :], q_ref[kv_head, 1, rows, :]
        full_s = scores(high_q, keys_at(kv_head, 0, middle + 1))
        high_s = [full_s[:, t * tile : (t + 1) * tile] for t in range(middle + 1)]
        high_s[middle] = masked(high_s[middle], middle, high_pos)
        low_s = masked(scores(low_q, keys_at(kv_head, 0, 1)), 0, low_pos)
        high_m = top(high_s)
        low_m = top([low_s])
        extra_s = []
        for j, is_low, key_tile, limit in extras:
            keys = jnp.where(
                is_low, keys_at(kv_head, j, j + 1), keys_at(kv_head, tiles - j, tiles - j + 1)
            )
            s = masked(scores(jnp.where(is_low, low_q, high_q), keys), key_tile, limit)
            m = top([s])
            low_m = jnp.where(is_low, jnp.maximum(low_m, m), low_m)
            high_m = jnp.where(is_low, high_m, jnp.maximum(high_m, m))
            extra_s.append(s)
        return high_s, low_s, extra_s, high_m, low_m

    def weigh(at, kv_head, heads, high_s, low_s, extra_s, high_m, low_m):
        high_o = weighted(
            jnp.concatenate([expo_of(s, high_m) for s in high_s], axis=1),
            values_at(kv_head, 0, middle + 1),
        )
        low_o = weighted(expo_of(low_s, low_m), values_at(kv_head, 0, 1))
        for (j, is_low, _, _), s in zip(extras, extra_s):
            rows_v = jnp.where(
                is_low, values_at(kv_head, j, j + 1), values_at(kv_head, tiles - j, tiles - j + 1)
            )
            o = weighted(expo_of(s, jnp.where(is_low, low_m, high_m)), rows_v)
            low_o = low_o + jnp.where(is_low, o, 0.0)
            high_o = high_o + jnp.where(is_low, 0.0, o)
        for side, (o, m) in enumerate(((low_o, low_m), (high_o, high_m))):
            out = slice(heads[0] * span, (heads[-1] + 1) * span)
            sum_ref[at, side, out] = o[:, :HEAD]
            total_ref[at, side, out] = o[:, HEAD:]
            top_ref[at, side, out] = jnp.broadcast_to(m, (o.shape[0], HEAD))

    cuts = max(1, CUTS - len(kv_list) + 1)
    many = -(-group // cuts)
    units = [
        (at, kv_head, range(first, min(group, first + many)))
        for at, kv_head in enumerate(kv_list)
        for first in range(0, group, many)
    ]
    scored = [score_all(kv_head, heads) for _, kv_head, heads in units]
    for unit, found in zip(units, scored):
        weigh(*unit, *found)


def finish_kernel(early, final, lacks, stages, span, group, kv_heads, q_ref, table, tail, *refs):
    final_ref = refs[0]
    states = refs[1 : 1 + 3 * len(stages)]
    out_ref, ready, sems = refs[1 + 3 * len(stages) :]
    in_order, low_pos, high_pos = own_blocks(table)
    first, second = blocks_of(final, table)
    final_in_order = first < second

    def bias_of(blocks, limit):
        lane_block = lax.broadcasted_iota(jnp.int32, (8, span * len(blocks)), 1) // span
        position = jnp.full(lane_block.shape, -1, jnp.int32)
        for number, block in enumerate(blocks):
            if block is not None:
                position = jnp.where(lane_block == number, block, position)
        return jnp.where(position < limit, 0.0, -jnp.inf)

    spots, biases = [], []
    for lack in lacks:
        held_first = min(early.index(number) for number in lack if number != final)
        ordered = early[held_first:] + [final]
        pairs = [blocks_of(number, table) for number in ordered]
        lower = [jnp.minimum(*pair) for pair in pairs]
        higher = [jnp.maximum(*pair) for pair in pairs]
        spots.append(held_first * span)
        biases.append((bias_of(lower, low_pos), bias_of([None] * len(lower) + higher, high_pos)))

    def rows_of(stage, part):
        columns = slice(part * HEAD, (part + 1) * HEAD)
        slots = [final_ref[slot * span : (slot + 1) * span, columns] for slot in range(2)]
        low = jnp.where(final_in_order, slots[0], slots[1])
        high = jnp.where(final_in_order, slots[1], slots[0])
        start = spots[stage]
        return (
            jnp.concatenate([tail[part, 0, start:, :], low], axis=0),
            jnp.concatenate([tail[part, 1, start:, :], high], axis=0),
        )

    where = [(stage, at) for stage, kv_list in enumerate(stages) for at in range(len(kv_list))]

    def score(kv_head):
        stage, at = where[kv_head]
        low_k, high_k = rows_of(stage, kv_head)
        keys = (low_k, jnp.concatenate([low_k, high_k], axis=0))
        found = []
        for side in range(2):
            s = lax.dot_general(
                q_ref[kv_head, side],
                keys[side],
                (((1,), (1,)), ((), ())),
                preferred_element_type=jnp.float32,
            )
            bias = biases[stage][side]
            clear = low_k.shape[0] if side and low_k.shape[0] % HEAD == 0 else 0
            part = s[:, clear:]
            part = (part.reshape(-1, 8, part.shape[1]) + bias[None, :, clear:]).reshape(part.shape)
            s = jnp.concatenate([s[:, :clear], part], axis=1) if clear else part
            new_m = jnp.maximum(
                states[3 * stage + 1][at, side], jnp.max(s, axis=-1, keepdims=True)
            )
            wide = jnp.concatenate([new_m] * -(-s.shape[1] // HEAD), axis=1)[:, : s.shape[1]]
            e = jnp.exp2((s - wide) * SCALE).astype(jnp.bfloat16)
            found.append((e, new_m))
        return found

    def merge(kv_head, found):
        stage, at = where[kv_head]
        sum_ref, top_ref, total_ref = states[3 * stage : 3 * stage + 3]
        low_v, high_v = rows_of(stage, kv_heads + kv_head)
        low_v = jnp.concatenate([low_v, jnp.ones(low_v.shape, low_v.dtype)], axis=1)
        high_v = jnp.concatenate([high_v, jnp.ones(high_v.shape, high_v.dtype)], axis=1)
        rows_v = (low_v, jnp.concatenate([low_v, high_v], axis=0))
        normed = []
        for side, (e, new_m) in enumerate(found):
            fade = jnp.exp2((top_ref[at, side] - new_m) * SCALE)
            more = jnp.dot(e, rows_v[side], preferred_element_type=jnp.float32)
            o = sum_ref[at, side] * fade + more[:, :HEAD]
            l = total_ref[at, side] * fade + more[:, HEAD:]
            normed.append((o / l).astype(jnp.bfloat16))
        low, high = normed
        for slot, rows in enumerate(
            (jnp.where(in_order, low, high), jnp.where(in_order, high, low))
        ):
            for g in range(group):
                ready[slot * span : (slot + 1) * span, head_columns(kv_head, g, group)] = rows[
                    g * span : (g + 1) * span
                ]
        columns = pl.ds(kv_head * group * HEAD, group * HEAD)
        copy = pltpu.make_async_copy(ready.at[:, columns], out_ref.at[:, columns], sems.at[kv_head])
        copy.start()
        return copy

    scored = [score(kv_head) for kv_head in range(kv_heads)]
    copies = [merge(kv_head, scored[kv_head]) for kv_head in range(kv_heads)]
    for copy in copies:
        copy.wait()


def attended(queries, keys, values, span_order):
    rows = queries.shape[0]
    span = rows // 2
    kv_heads = keys.shape[1] // HEAD
    group = queries.shape[1] // (kv_heads * HEAD)
    size = lax.axis_size("blk")
    far = size // CORES // 2
    count = rows * size
    vmem = pl.BlockSpec(memory_space=pltpu.VMEM)
    anywhere = pl.BlockSpec(memory_space=pltpu.HBM)
    params = pltpu.CompilerParams(vmem_limit_bytes=8 * 2**20 + 6 * count * 2 * kv_heads * HEAD)

    def call(kernel, out_shape, in_specs, **extra):
        return pl.pallas_call(
            kernel, out_shape=out_shape, in_specs=in_specs, compiler_params=params, **extra
        )

    width = keys.shape[1]
    lowest = jnp.array(-jnp.inf, keys.dtype)
    mine = jnp.maximum(
        lax.pad(keys, lowest, ((0, 0, 0), (0, width, 0))),
        lax.pad(values, lowest, ((0, 0, 0), (width, 0, 0))),
    )
    pieces = gather(mine)
    plan = [p[1:] for p in pieces]
    table_rows = -(-2 * len(plan) // LANES)
    table = call(
        functools.partial(setup_kernel, plan),
        jax.ShapeDtypeStruct((table_rows, LANES), jnp.int32),
        [vmem],
        out_specs=vmem,
    )(span_order.reshape(1, -1))
    q_held = call(
        functools.partial(load_kernel, span, group),
        jax.ShapeDtypeStruct((kv_heads, 2, group * span, HEAD), queries.dtype),
        [vmem, vmem],
        out_specs=vmem,
    )(table, queries)
    lacks = [
        [n for n, e in enumerate(plan) if e[0] == far or (e[0] == far - 1 and not e[3])],
        [n for n, e in enumerate(plan) if e[0] == far],
    ]
    stages = [list(range(kv_heads - 1)), list(range(kv_heads - 1, kv_heads))]
    held_shape = jax.ShapeDtypeStruct((2 * kv_heads + 1, count, HEAD), jnp.bfloat16)
    held = None
    states = []

    def place(numbers, held):
        kernel = (
            functools.partial(place_first, numbers, lacks[0], span)
            if held is None
            else functools.partial(place_more, numbers, span)
        )
        before = [] if held is None else [held]
        extra = {} if held is None else {"input_output_aliases": {1: 0}}
        return call(
            kernel, held_shape, [vmem] * (1 + len(before) + len(numbers)), out_specs=vmem, **extra
        )(table, *before, *[pieces[number][0] for number in numbers])

    def attend(stage, held):
        shape = jax.ShapeDtypeStruct((len(stages[stage]), 2, group * span, HEAD), jnp.float32)
        return call(
            functools.partial(attend_kernel, stages[stage], span, group),
            (shape, shape, shape),
            [vmem, vmem, vmem],
            out_specs=(vmem, vmem, vmem),
        )(q_held, table, held)

    placed = set(lacks[0])
    for step in range(2, far + 1):
        numbers = []
        for number, entry in enumerate(plan):
            ready = step == far or entry[0] < step - 1 or (entry[0] == step - 1 and entry[3])
            if ready and number not in placed:
                numbers.append(number)
        placed.update(numbers)
        held = place(numbers, held)
    states += attend(0, held)
    rest = [number for number in lacks[0] if number not in lacks[1]]
    final = next(number for number in lacks[1] if not plan[number][3])
    early = rest + [number for number in lacks[1] if number != final]
    held, tail = call(
        functools.partial(place_last, rest, early, span),
        (
            held_shape,
            jax.ShapeDtypeStruct((2 * kv_heads, 2, len(early) * span, HEAD), jnp.bfloat16),
        ),
        [vmem] * (2 + len(early)),
        out_specs=(vmem, vmem),
        input_output_aliases={1: 0},
    )(table, held, *[pieces[number][0] for number in early])
    states += attend(1, held)
    return call(
        functools.partial(finish_kernel, early, final, lacks, stages, span, group, kv_heads),
        jax.ShapeDtypeStruct(queries.shape, jnp.bfloat16),
        [vmem] * (4 + len(states)),
        out_specs=anywhere,
        scratch_shapes=[
            pltpu.VMEM(queries.shape, jnp.bfloat16),
            pltpu.SemaphoreType.DMA((kv_heads,)),
        ],
    )(q_held, table, tail, pieces[final][0], *states)


def solution(mesh):
    return jax.shard_map(
        attended,
        mesh=mesh,
        in_specs=(
            P(("parts", "blk"), None),
            P(("parts", "blk"), None),
            P(("parts", "blk"), None),
            P("parts"),
        ),
        out_specs=P(("parts", "blk"), None),
        check_vma=False,
    )
```

```python
import functools
import math

import jax
import jax.numpy as jnp
from jax import lax
from jax.experimental import pallas as pl
from jax.experimental.pallas import tpu as pltpu
from jax.sharding import PartitionSpec as P


HEAD = 128
CORES = 2
TILE_SPANS = 8
LANES = 128
CUTS = 2
SCALE = math.log2(math.e) / HEAD**0.5


def chip_at(place, chips):
    half = chips // 2
    return 2 * place if place < half else 2 * (chips - 1 - place) + 1


def place_of(chip, chips):
    return chip // 2 if chip % 2 == 0 else chips - 1 - chip // 2


def ring_pairs(size, sender, receiver, hops):
    chips = size // CORES
    pairs = []
    for device in range(size):
        chip, core = device // CORES, device % CORES
        ahead = core == sender
        place = (place_of(chip, chips) + (hops if ahead else -hops)) % chips
        target = receiver if ahead else 1 - receiver
        pairs.append((device, chip_at(place, chips) * CORES + target))
    return pairs


def mate_pairs(size):
    return [(device, device ^ 1) for device in range(size)]


def gather(mine):
    size = lax.axis_size("blk")
    far = size // CORES // 2

    def swap(array):
        return lax.ppermute(array, "blk", mate_pairs(size))

    def send(array, sender, receiver, hops):
        return lax.ppermute(array, "blk", ring_pairs(size, sender, receiver, hops))

    mate = swap(mine)
    pieces = [(mine, 0, 0, 0, True), (mate, 0, 0, 0, False)]
    lead = follow = None
    held = 0
    for step in range(1, far + 1):
        for rest in range(2 if step < far else 1):
            source = (mate if rest else mine) if step == 1 else (follow if rest else lead)
            got = send(source, held, 1 - held, 1)
            if rest:
                follow = got
            else:
                lead = got
            pieces.append((got, step, 1 - held, rest, True))
            pieces.append((swap(got), step, 1 - held, rest, False))
        held = 1 - held
    return pieces


def ring_spot(size):
    chips = size // CORES
    mine = lax.axis_index("blk")
    chip = mine // CORES
    place = jnp.where(chip % 2 == 0, chip // 2, chips - 1 - chip // 2)
    return mine, chip, mine % CORES, place, chips


def device_of(entry):
    distance, behind, rest, own = entry
    _, chip, core, place, chips = ring_spot(lax.axis_size("blk"))
    half = chips // 2
    holder = core if own else 1 - core
    if distance == 0:
        return chip * CORES + holder
    from_behind = (holder == behind).astype(jnp.int32)
    spot = (place + chips + distance - 2 * distance * from_behind) % chips
    from_chip = jnp.where(spot < half, 2 * spot, 2 * (chips - 1 - spot) + 1)
    return from_chip * CORES + rest + (1 - 2 * rest) * (1 - from_behind)


def blocks_of(piece, table):
    return [table[at // LANES, at % LANES] for at in (2 * piece, 2 * piece + 1)]


def own_blocks(table):
    first, second = blocks_of(0, table)
    in_order = first < second
    return in_order, jnp.minimum(first, second), jnp.maximum(first, second)


def setup_kernel(plan, order_ref, table):
    rows = table.shape[0]
    at = lax.broadcasted_iota(jnp.int32, (rows, LANES), 0) * LANES + lax.broadcasted_iota(
        jnp.int32, (rows, LANES), 1
    )
    wanted = jnp.zeros((rows, LANES), jnp.int32)
    for number, entry in enumerate(plan):
        device = device_of(entry)
        for slot in range(2):
            wanted = jnp.where(at == 2 * number + slot, device * 2 + slot, wanted)
    known = jnp.zeros((rows, LANES), jnp.int32)
    for block in range(order_ref.shape[1]):
        known = jnp.where(wanted == block, order_ref[0, block], known)
    table[...] = known


def load_kernel(span, group, table, q_ref, q_out):
    in_order, _, _ = own_blocks(table)
    for kv_head in range(q_out.shape[0]):
        for g in range(group):
            columns = head_columns(kv_head, g, group)
            slots = [q_ref[slot * span : (slot + 1) * span, columns] for slot in range(2)]
            rows = slice(g * span, (g + 1) * span)
            q_out[kv_head, 0, rows, :] = jnp.where(in_order, slots[0], slots[1])
            q_out[kv_head, 1, rows, :] = jnp.where(in_order, slots[1], slots[0])


def put_block(held, block, span, rows, present):
    at = pl.ds(pl.multiple_of(block * span, span), span)
    parts = held.shape[0] - 1
    for part in range(parts):
        held[part, at, :] = rows(part)
    held[parts, at, :] = jnp.full((span, HEAD), present, held.dtype)


def place_kernel(numbers, span, table, pieces, held):
    for number, ref in zip(numbers, pieces):
        for slot, block in enumerate(blocks_of(number, table)):
            put_block(
                held,
                block,
                span,
                lambda part: ref[slot * span : (slot + 1) * span, part * HEAD : (part + 1) * HEAD],
                1.0,
            )


def place_first(numbers, missing, span, table, *refs):
    *pieces, held = refs
    mine = pieces[0]
    in_order, _, _ = own_blocks(table)
    keys = (held.shape[0] - 1) // 2

    def stand_in(part):
        if part >= keys:
            return jnp.zeros((span, HEAD), held.dtype)
        columns = slice(part * HEAD, (part + 1) * HEAD)
        both = [mine[slot * span : slot * span + 1, columns].astype(jnp.float32) for slot in range(2)]
        row = jnp.where(in_order, both[0], both[1])
        return jnp.broadcast_to(row, (span, HEAD)).astype(held.dtype)

    fills = [stand_in(part) for part in range(2 * keys)]
    for number in missing:
        for block in blocks_of(number, table):
            put_block(held, block, span, lambda part: fills[part], 0.0)
    place_kernel(numbers, span, table, pieces, held)


def place_more(numbers, span, table, held_in, *refs):
    del held_in
    *pieces, held = refs
    place_kernel(numbers, span, table, pieces, held)


def head_columns(kv_head, g, group):
    return slice((kv_head * group + g) * HEAD, (kv_head * group + g + 1) * HEAD)


def attend_kernel(kv_list, span, group, q_ref, table, held, sum_ref, top_ref, total_ref):
    kv_heads = (held.shape[0] - 1) // 2
    tile = TILE_SPANS * span
    tiles = held.shape[1] // tile
    middle = tiles // 2
    _, low_pos, high_pos = own_blocks(table)
    gap = lax.broadcasted_iota(jnp.int32, (span, tile), 1) - lax.broadcasted_iota(
        jnp.int32, (span, tile), 0
    )
    reach = low_pos // TILE_SPANS

    def masked(raw, key_tile, limit):
        keep = gap <= limit * span - key_tile * tile
        return jnp.where(keep[None], raw.reshape(-1, span, tile), -jnp.inf).reshape(raw.shape)

    def scores(query, keys):
        return lax.dot_general(
            query, keys, (((1,), (1,)), ((), ())), preferred_element_type=jnp.float32
        )

    def weighted(expo, rows_v):
        return jnp.dot(expo.astype(jnp.bfloat16), rows_v, preferred_element_type=jnp.float32)

    def top(items):
        return jnp.max(functools.reduce(jnp.maximum, items), axis=-1, keepdims=True)

    def expo_of(s, m):
        return jnp.exp2((s - m) * SCALE)

    def keys_at(kv_head, first, last):
        return held[kv_head, first * tile : last * tile, :]

    def values_at(kv_head, first, last):
        rows = slice(first * tile, last * tile)
        return jnp.concatenate([held[kv_heads + kv_head, rows, :], held[2 * kv_heads, rows, :]], 1)

    extras = []
    for j in range(1, middle):
        is_low = reach >= j
        extras.append(
            (j, is_low, jnp.where(is_low, j, tiles - j), jnp.where(is_low, low_pos, high_pos))
        )

    def score_all(kv_head, heads):
        rows = slice(heads[0] * span, (heads[-1] + 1) * span)
        low_q, high_q = q_ref[kv_head, 0, rows, :], q_ref[kv_head, 1, rows, :]
        full_s = scores(high_q, keys_at(kv_head, 0, middle + 1))
        high_s = [full_s[:, t * tile : (t + 1) * tile] for t in range(middle + 1)]
        high_s[middle] = masked(high_s[middle], middle, high_pos)
        low_s = masked(scores(low_q, keys_at(kv_head, 0, 1)), 0, low_pos)
        high_m = top(high_s)
        low_m = top([low_s])
        extra_s = []
        for j, is_low, key_tile, limit in extras:
            keys = jnp.where(
                is_low, keys_at(kv_head, j, j + 1), keys_at(kv_head, tiles - j, tiles - j + 1)
            )
            s = masked(scores(jnp.where(is_low, low_q, high_q), keys), key_tile, limit)
            m = top([s])
            low_m = jnp.where(is_low, jnp.maximum(low_m, m), low_m)
            high_m = jnp.where(is_low, high_m, jnp.maximum(high_m, m))
            extra_s.append(s)
        return high_s, low_s, extra_s, high_m, low_m

    def weigh(at, kv_head, heads, high_s, low_s, extra_s, high_m, low_m):
        high_o = weighted(
            jnp.concatenate([expo_of(s, high_m) for s in high_s], axis=1),
            values_at(kv_head, 0, middle + 1),
        )
        low_o = weighted(expo_of(low_s, low_m), values_at(kv_head, 0, 1))
        for (j, is_low, _, _), s in zip(extras, extra_s):
            rows_v = jnp.where(
                is_low, values_at(kv_head, j, j + 1), values_at(kv_head, tiles - j, tiles - j + 1)
            )
            o = weighted(expo_of(s, jnp.where(is_low, low_m, high_m)), rows_v)
            low_o = low_o + jnp.where(is_low, o, 0.0)
            high_o = high_o + jnp.where(is_low, 0.0, o)
        for side, (o, m) in enumerate(((low_o, low_m), (high_o, high_m))):
            out = slice(heads[0] * span, (heads[-1] + 1) * span)
            sum_ref[at, side, out] = o[:, :HEAD]
            total_ref[at, side, out] = o[:, HEAD:]
            top_ref[at, side, out] = jnp.broadcast_to(m, (o.shape[0], HEAD))

    cuts = max(1, CUTS - len(kv_list) + 1)
    many = -(-group // cuts)
    units = [
        (at, kv_head, range(first, min(group, first + many)))
        for at, kv_head in enumerate(kv_list)
        for first in range(0, group, many)
    ]
    scored = [score_all(kv_head, heads) for _, kv_head, heads in units]
    for unit, found in zip(units, scored):
        weigh(*unit, *found)


def finish_kernel(numbers, lacks, stages, span, group, kv_heads, q_ref, table, *refs):
    pieces = dict(zip(numbers, refs))
    states = refs[len(numbers) : len(numbers) + 3 * len(stages)]
    out_ref, ready, sems = refs[len(numbers) + 3 * len(stages) :]
    in_order, *positions = own_blocks(table)
    width = kv_heads * HEAD
    biases = []
    for lack in lacks:
        blocks = [block for number in lack for block in blocks_of(number, table)]
        lane_block = lax.broadcasted_iota(jnp.int32, (8, span * len(blocks)), 1) // span
        position = jnp.zeros(lane_block.shape, jnp.int32)
        for number, block in enumerate(blocks):
            position = jnp.where(lane_block == number, block, position)
        biases.append([jnp.where(position < pos, 0.0, -jnp.inf) for pos in positions])

    def rows_of(stage, column):
        parts = [pieces[number][:, column : column + HEAD] for number in lacks[stage]]
        return jnp.concatenate(parts, axis=0)

    where = [(stage, at) for stage, kv_list in enumerate(stages) for at in range(len(kv_list))]
    copies = []
    for kv_head, (stage, at) in enumerate(where):
        sum_ref, top_ref, total_ref = states[3 * stage : 3 * stage + 3]
        queries = [q_ref[kv_head, side] for side in range(2)]
        rows_k = rows_of(stage, kv_head * HEAD)
        rows_v = rows_of(stage, width + kv_head * HEAD)
        rows_v = jnp.concatenate([rows_v, jnp.ones(rows_v.shape, rows_v.dtype)], axis=1)
        normed = []
        for side in range(2):
            s = lax.dot_general(
                queries[side], rows_k, (((1,), (1,)), ((), ())), preferred_element_type=jnp.float32
            )
            s = (s.reshape(-1, 8, s.shape[1]) + biases[stage][side][None]).reshape(s.shape)
            m = top_ref[at, side]
            new_m = jnp.maximum(m, jnp.max(s, axis=-1, keepdims=True))
            wide = jnp.concatenate([new_m] * (s.shape[1] // HEAD), axis=1)
            e = jnp.exp2((s - wide) * SCALE).astype(jnp.bfloat16)
            fade = jnp.exp2((m - new_m) * SCALE)
            more = jnp.dot(e, rows_v, preferred_element_type=jnp.float32)
            o = sum_ref[at, side] * fade + more[:, :HEAD]
            l = total_ref[at, side] * fade + more[:, HEAD:]
            normed.append((o / l).astype(jnp.bfloat16))
        low, high = normed
        for slot, rows in enumerate(
            (jnp.where(in_order, low, high), jnp.where(in_order, high, low))
        ):
            for g in range(group):
                ready[slot * span : (slot + 1) * span, head_columns(kv_head, g, group)] = rows[
                    g * span : (g + 1) * span
                ]
        columns = pl.ds(kv_head * group * HEAD, group * HEAD)
        copy = pltpu.make_async_copy(ready.at[:, columns], out_ref.at[:, columns], sems.at[kv_head])
        copy.start()
        copies.append(copy)
    for copy in copies:
        copy.wait()


def attended(queries, keys, values, span_order):
    rows = queries.shape[0]
    span = rows // 2
    kv_heads = keys.shape[1] // HEAD
    group = queries.shape[1] // (kv_heads * HEAD)
    size = lax.axis_size("blk")
    far = size // CORES // 2
    count = rows * size
    vmem = pl.BlockSpec(memory_space=pltpu.VMEM)
    anywhere = pl.BlockSpec(memory_space=pltpu.HBM)
    params = pltpu.CompilerParams(vmem_limit_bytes=8 * 2**20 + 6 * count * 2 * kv_heads * HEAD)

    def call(kernel, out_shape, in_specs, **extra):
        return pl.pallas_call(
            kernel, out_shape=out_shape, in_specs=in_specs, compiler_params=params, **extra
        )

    width = keys.shape[1]
    lowest = jnp.array(-jnp.inf, keys.dtype)
    mine = jnp.maximum(
        lax.pad(keys, lowest, ((0, 0, 0), (0, width, 0))),
        lax.pad(values, lowest, ((0, 0, 0), (width, 0, 0))),
    )
    pieces = gather(mine)
    plan = [p[1:] for p in pieces]
    table_rows = -(-2 * len(plan) // LANES)
    table = call(
        functools.partial(setup_kernel, plan),
        jax.ShapeDtypeStruct((table_rows, LANES), jnp.int32),
        [vmem],
        out_specs=vmem,
    )(span_order.reshape(1, -1))
    q_held = call(
        functools.partial(load_kernel, span, group),
        jax.ShapeDtypeStruct((kv_heads, 2, group * span, HEAD), queries.dtype),
        [vmem, vmem],
        out_specs=vmem,
    )(table, queries)
    lacks = [
        [n for n, e in enumerate(plan) if e[0] == far or (e[0] == far - 1 and not e[3])],
        [n for n, e in enumerate(plan) if e[0] == far],
    ]
    stages = [list(range(kv_heads // 2)), list(range(kv_heads // 2, kv_heads))]
    held_shape = jax.ShapeDtypeStruct((2 * kv_heads + 1, count, HEAD), jnp.bfloat16)
    held = None
    states = []

    def place(numbers, held):
        kernel = (
            functools.partial(place_first, numbers, lacks[0], span)
            if held is None
            else functools.partial(place_more, numbers, span)
        )
        before = [] if held is None else [held]
        extra = {} if held is None else {"input_output_aliases": {1: 0}}
        return call(
            kernel, held_shape, [vmem] * (1 + len(before) + len(numbers)), out_specs=vmem, **extra
        )(table, *before, *[pieces[number][0] for number in numbers])

    def attend(stage, held):
        shape = jax.ShapeDtypeStruct((len(stages[stage]), 2, group * span, HEAD), jnp.float32)
        return call(
            functools.partial(attend_kernel, stages[stage], span, group),
            (shape, shape, shape),
            [vmem, vmem, vmem],
            out_specs=(vmem, vmem, vmem),
        )(q_held, table, held)

    placed = set(lacks[0])
    for step in range(2, far + 1):
        numbers = []
        for number, entry in enumerate(plan):
            ready = step == far or entry[0] < step - 1 or (entry[0] == step - 1 and entry[3])
            if ready and number not in placed:
                numbers.append(number)
        placed.update(numbers)
        held = place(numbers, held)
    states += attend(0, held)
    rest = [number for number in lacks[0] if number not in lacks[1]]
    held = place(rest, held)
    states += attend(1, held)
    numbers = lacks[0]
    return call(
        functools.partial(finish_kernel, numbers, lacks, stages, span, group, kv_heads),
        jax.ShapeDtypeStruct(queries.shape, jnp.bfloat16),
        [vmem] * (2 + len(numbers) + len(states)),
        out_specs=anywhere,
        scratch_shapes=[
            pltpu.VMEM(queries.shape, jnp.bfloat16),
            pltpu.SemaphoreType.DMA((kv_heads,)),
        ],
    )(q_held, table, *[pieces[number][0] for number in numbers], *states)


def solution(mesh):
    return jax.shard_map(
        attended,
        mesh=mesh,
        in_specs=(
            P(("parts", "blk"), None),
            P(("parts", "blk"), None),
            P(("parts", "blk"), None),
            P("parts"),
        ),
        out_specs=P(("parts", "blk"), None),
        check_vma=False,
    )
```
